32 devices in a mesh: row: 8 (over y, x, core), col: 4 (over z).
Axes of the slice: x: 2, y: 2, z: 4, core: 2. Of those that a mesh axis runs over, the one named last changes fastest.
Arguments:
- tokens: bfloat16 [32, 8192], P(None, 'row'), may hold values from -6 to 6
- gain: float32 [8192], P('row'), may hold values from 0.24 to 4.5
- gate_weight: bfloat16 [8192, 28672], P('row', 'col'), may hold values from -0.0625 to 0.0625
- up_weight: bfloat16 [8192, 28672], P('row', 'col'), may hold values from -0.0625 to 0.0625
- down_weight: bfloat16 [28672, 8192], P('col', 'row'), may hold values from -0.03125 to 0.03125
- probes: float32 [4, 32, 8192], P(None, None, 'row'), may hold values from -6 to 6
Outputs:
- basis: float32 [4, 32, 8192], P(None, None, 'row')
- stretch: float32 [4], replicated
The draws below stay inside these ranges and needn't reach their ends.
All inputs are finite; a program needn't handle non-finite values.
Results may differ from the reference program's by a relative error of at most 0.0085.
Values may be sent and summed in bfloat16 or wider, within the bound.
No kernel may reach another device: no remote copies, remote signals or barrier semaphores. Data moves between devices by JAX's collectives and lax.ppermute only.
A program may use at most 128 MiB of HBM per device.

```python
import jax
import jax.numpy as jnp
from jax import lax

D = 8192
FF = 28672
TOKENS = 32
PROBES = 4
ITERS = 3


def draw_gain(key, part):
    position = jnp.arange(D, dtype=jnp.float32) / max(D - 1, 1)
    jitter = jax.random.uniform(jax.random.fold_in(key, 11), (D,), jnp.float32, 0.8, 1.25)
    return 0.55 * jnp.power(3.0, position) * jitter


def levels(rng, extent, split, low, top_value):
    factor_of = 1.0
    for axis_at, shards_of in split:
        steps = jax.random.uniform(jax.random.fold_in(jax.random.fold_in(rng, 6), axis_at), (shards_of,), jnp.float32, low / len(split), top_value / len(split))
        factor_of = factor_of * jnp.repeat(jnp.exp(steps), extent[axis_at] // shards_of).reshape((-1,) + (1,) * (len(extent) - 1 - axis_at))
    return factor_of


def bell_draw(own_key, dims, deviation, most, cuts=(), held_as=jnp.bfloat16):
    result = deviation * jax.random.normal(own_key, dims, jnp.float32)
    if cuts:
        result = result * levels(own_key, dims, cuts, -0.22, 0.18)
    return jnp.clip(result, -most, most).astype(held_as)


def setup_inputs(seed: int = 0) -> dict:
    key_list = jax.random.split(jax.random.key(seed), 7)
    tokens = bell_draw(key_list[0], (TOKENS, D), 1.0, 6.0, ((1, 8),))
    gain = draw_gain(jax.random.fold_in(key_list[6], 71), 0)
    gate_weight = bell_draw(key_list[2], (D, FF), D ** -0.5, 0.0625, ((0, 8), (1, 4)))
    up_weight = bell_draw(key_list[3], (D, FF), D ** -0.5, 0.0625, ((0, 8), (1, 4)))
    down_weight = bell_draw(key_list[4], (FF, D), FF ** -0.5, 0.03125, ((0, 4), (1, 8)))
    probes = bell_draw(key_list[5], (PROBES, TOKENS, D), 1.0, 6.0, ((2, 8),), jnp.float32)
    return {"tokens": tokens, "gain": gain, "gate_weight": gate_weight, "up_weight": up_weight, "down_weight": down_weight, "probes": probes}


epsilon = 1e-06

def reference(tokens, gain, gate_weight, up_weight, down_weight, probes):
    scaled = (tokens.astype(jnp.float32) * gain).astype(jnp.bfloat16)
    gate = jnp.dot(scaled, gate_weight, preferred_element_type=jnp.float32)
    up = jnp.dot(scaled, up_weight, preferred_element_type=jnp.float32)
    sigmoid_gate = 1.0 / (1.0 + jnp.exp(-gate))
    activated = gate * sigmoid_gate
    slope = sigmoid_gate * (1.0 + gate * (1.0 - sigmoid_gate)) * up
    slope_all = jnp.tile(slope, (PROBES, 1))
    activated_all = jnp.tile(activated, (PROBES, 1))
    current = probes
    level = jnp.zeros((PROBES,), jnp.float32)
    for sweep in range(ITERS):
        pushed = (current * gain).astype(jnp.bfloat16).reshape(PROBES * TOKENS, D)
        gate_tan = jnp.dot(pushed, gate_weight, preferred_element_type=jnp.float32)
        up_tan = jnp.dot(pushed, up_weight, preferred_element_type=jnp.float32)
        hidden = (slope_all * gate_tan + activated_all * up_tan).astype(jnp.bfloat16)
        tangent = jnp.dot(hidden, down_weight, preferred_element_type=jnp.float32).astype(jnp.bfloat16)
        back = jnp.dot(tangent, down_weight.T, preferred_element_type=jnp.float32).astype(jnp.bfloat16)
        gate_pull = (slope_all * back).astype(jnp.bfloat16)
        up_pull = (activated_all * back).astype(jnp.bfloat16)
        pulled = jnp.dot(gate_pull, gate_weight.T, preferred_element_type=jnp.float32)
        pulled = pulled + jnp.dot(up_pull, up_weight.T, preferred_element_type=jnp.float32)
        grown = pulled.reshape(PROBES, TOKENS, D) * gain
        level = lax.optimization_barrier(jnp.mean(grown * grown, axis=(1, 2)))
        current = grown * lax.rsqrt(level + epsilon)[:, None, None]
    return (current, jnp.sqrt(level))
```

```python
import functools

import jax
import jax.numpy as jnp
from jax import lax
from jax.experimental import pallas as pl
from jax.experimental.pallas import tpu as pltpu
from jax.sharding import PartitionSpec as P

ITERS = 3
EPSILON = 1e-06
SUB = 8
CHUNKS = 2
F32 = jnp.float32
BF16 = jnp.bfloat16
TRANSPOSED = (((1,), (1,)), ((), ()))


def swap(x, axis, mask):
    n = lax.axis_size(axis)
    return lax.ppermute(x, axis, [(i, i ^ mask) for i in range(n)])


def stack_rows(pieces):
    if len(pieces) == 1:
        return pieces[0]
    if pieces[0].shape[0] % 16 == 0 or pieces[0].dtype == F32:
        return jnp.concatenate(pieces, axis=0)
    return jnp.concatenate([p.astype(F32) for p in pieces], axis=0).astype(pieces[0].dtype)


class Layout:
    def __init__(self, probes, tokens, ranks, cols):
        self.probes, self.tokens, self.ranks, self.cols = probes, tokens, ranks, cols
        self.rows = probes * tokens
        self.q = tokens // SUB
        self.h = ranks // self.q
        self.low = probes // self.h
        self.half = self.rows // self.h
        self.block = self.rows // ranks
        self.zrows = self.rows // cols


def any_spec():
    return pl.BlockSpec(memory_space=pl.ANY)


def call(body, name, ins, outs, scratch, flops, moved, direct=0):
    vmem = pl.BlockSpec(memory_space=pltpu.VMEM)
    return pl.pallas_call(
        body,
        in_specs=[any_spec()] * len(ins),
        out_specs=[any_spec()] * direct + [vmem] * (len(outs) - direct),
        out_shape=outs,
        scratch_shapes=scratch,
        compiler_params=pltpu.CompilerParams(vmem_limit_bytes=48 * 2**20),
        cost_estimate=pl.CostEstimate(flops=flops, bytes_accessed=moved, transcendentals=0),
        name=name,
    )(*ins)


def tile_of(extent):
    return max(t for t in range(128, 1025, 128) if extent % t == 0)


def split_of(count, chunks):
    chunks = min(chunks, count)
    ends = [-(-count * (j + 1) // chunks) for j in range(chunks)]
    return list(zip([0] + ends[:-1], ends))


def spread(lay, per_token):
    return per_token.reshape(1, lay.q, 1, SUB, per_token.shape[-1])


def start_all(copies):
    for copy in copies:
        copy.start()
    return copies


def wait_all(copies):
    for copy in copies:
        copy.wait()


def load_rows(chunks, dest, sem):
    copies, col = [], 0
    for pieces in chunks:
        row, w = 0, pieces[0].shape[1]
        for p in pieces:
            n = p.shape[0]
            there = dest.at[pl.ds(row, n), pl.ds(col, w)]
            copies.append(pltpu.make_async_copy(p, there, sem.at[len(copies)]))
            row += n
        col += w
    return copies


def cols_of(i, t):
    return pl.ds(pl.multiple_of(i * t, t), t)


def each(start, stop, body):
    def step(i, carry):
        body(i)
        return carry

    lax.fori_loop(start, stop, step, 0)


def weight_copies(t, tables, sem, i):
    return [
        pltpu.make_async_copy(ref.at[:, cols_of(i, t)], dest.at[i], sem.at[i, k])
        for k, (ref, dest) in enumerate(tables)
    ]


def row_copies(t, ref, dest, sem, i):
    return [pltpu.make_async_copy(ref.at[cols_of(i, t), :], dest.at[i], sem.at[i])]


def store_copies(lay, t, start, halves, outs, sem, i):
    here = cols_of(i - start, t)
    return [
        pltpu.make_async_copy(v.at[i], o.at[:, here], sem.at[i, k])
        for k, (v, o) in enumerate(zip(halves, outs))
    ]


def fill(lay, halves, i, joined):
    for k, v in enumerate(halves):
        v[i] = joined[k * lay.half : (k + 1) * lay.half].astype(v.dtype)


def half_scratch(lay, tiles, t):
    return [pltpu.VMEM((tiles, lay.half, t), F32)] + [
        pltpu.VMEM((tiles, lay.half, t), BF16)
    ] * (lay.h - 1)


def push_body(lay, t, split, extra, *refs):
    x_ref, *tables = refs[:5]
    refs = refs[5:]
    sq_ref = refs[0] if extra else None
    refs = refs[extra:]
    outs = [refs[j * lay.h : (j + 1) * lay.h] for j in range(len(split))]
    refs = refs[len(split) * lay.h :]
    x_v, dests, sq_v, lev_v = refs[0], refs[1:5], refs[5], refs[6 : 6 + lay.h]
    halves = refs[6 + lay.h : 6 + 2 * lay.h]
    w_sem, in_sem, lev_sem, out_sem = refs[6 + 2 * lay.h :]
    count = split[-1][1]
    loads = functools.partial(weight_copies, t, list(zip(tables, dests)), w_sem)
    small = [pltpu.make_async_copy(x_ref, x_v, in_sem.at[0])]
    if extra:
        small.append(pltpu.make_async_copy(sq_ref, sq_v, in_sem.at[1]))
    start_all(small)
    each(0, count, lambda i: start_all(loads(i)) and None)
    wait_all(small)
    tail = []
    if extra:
        w = (split[0][1] - split[0][0]) * t
        for k, v in enumerate(lev_v):
            v[...] = sq_v[k * lay.half : (k + 1) * lay.half, :].astype(v.dtype)
            there = outs[0][k].at[:, pl.ds(w, 128)]
            tail.append(pltpu.make_async_copy(v, there, lev_sem.at[k]))
        start_all(tail)
    for (start, stop), group in zip(split, outs):

        def one(i, start=start, group=group):
            wait_all(loads(i))
            x = x_v[...]
            wg_v, wu_v, s_v, a_v = dests
            g = jnp.dot(x, wg_v[i], preferred_element_type=F32)
            u = jnp.dot(x, wu_v[i], preferred_element_type=F32)
            shape = (lay.h, lay.q, lay.low, SUB, t)
            s, a = spread(lay, s_v[i]), spread(lay, a_v[i])
            fill(lay, halves, i, (s * g.reshape(shape) + a * u.reshape(shape)).reshape(lay.rows, t))
            start_all(store_copies(lay, t, start, halves, group, out_sem, i))

        each(start, stop, one)
    for (start, stop), group in zip(split, outs):
        each(
            start,
            stop,
            lambda i, start=start, group=group: wait_all(
                store_copies(lay, t, start, halves, group, out_sem, i)
            ),
        )
    wait_all(tail)


def half_outs(lay, w):
    return [jax.ShapeDtypeStruct((lay.half, w), F32)] + [
        jax.ShapeDtypeStruct((lay.half, w), BF16)
    ] * (lay.h - 1)


def grouped(lay, outs):
    return [outs[j : j + lay.h] for j in range(0, len(outs), lay.h)]


def push(lay, x, wg, wu, slope, act, squares, chunks):
    depth, width = wg.shape
    t = tile_of(width)
    tiles = width // t
    split = split_of(tiles, chunks)
    extra = squares is not None
    outs = []
    for j, (start, stop) in enumerate(split):
        outs += half_outs(lay, (stop - start) * t + (128 if extra and j == 0 else 0))
    scratch = [
        pltpu.VMEM(x.shape, BF16),
        pltpu.VMEM((tiles, depth, t), BF16),
        pltpu.VMEM((tiles, depth, t), BF16),
        pltpu.VMEM((tiles, lay.tokens, t), F32),
        pltpu.VMEM((tiles, lay.tokens, t), F32),
        pltpu.VMEM((lay.rows, 128), F32),
        *[pltpu.VMEM((lay.half, 128), o.dtype) for o in outs[: lay.h]],
        *half_scratch(lay, tiles, t),
        pltpu.SemaphoreType.DMA((tiles, 4)),
        pltpu.SemaphoreType.DMA((2,)),
        pltpu.SemaphoreType.DMA((lay.h,)),
        pltpu.SemaphoreType.DMA((tiles, lay.h)),
    ]
    ins = [x, wg, wu, slope, act] + ([squares] if extra else [])
    body = functools.partial(push_body, lay, t, split, int(extra))
    flops, moved = 4 * lay.rows * depth * width, 4 * depth * width
    return grouped(lay, call(body, "push", ins, outs, scratch, flops, moved, direct=len(outs)))


def write_sum(lay, total, outs):
    outs[0][...] = total[: lay.zrows]
    for k, ref in enumerate(outs[1:], 1):
        ref[...] = total[k * lay.zrows : (k + 1) * lay.zrows].astype(BF16)


def sum_outs(lay, depth):
    return [jax.ShapeDtypeStruct((lay.zrows, depth), F32)] + [
        jax.ShapeDtypeStruct((lay.zrows, depth), BF16)
    ] * (lay.cols - 1)


def down_body(lay, t, tiles, counts, *refs):
    chunks = []
    for n in counts:
        chunks.append(refs[:n])
        refs = refs[n:]
    wd_ref, refs = refs[0], refs[1:]
    outs = refs[: lay.cols]
    x_v, w_v, acc, w_sem, in_sem = refs[lay.cols :]
    small = start_all(load_rows(chunks, x_v, in_sem))
    loads = functools.partial(row_copies, t, wd_ref, w_v, w_sem)
    each(0, tiles, lambda i: start_all(loads(i)) and None)
    acc[...] = jnp.zeros_like(acc)
    wait_all(small)

    def one(i):
        wait_all(loads(i))
        acc[...] += jnp.dot(x_v[:, cols_of(i, t)], w_v[i], preferred_element_type=F32)

    each(0, tiles, one)
    write_sum(lay, acc[...], outs)


def down(lay, chunks, wd):
    width, depth = wd.shape
    t = tile_of(width)
    tiles = width // t
    pieces = [p for c in chunks for p in c]
    scratch = [
        pltpu.VMEM((lay.rows, width), BF16),
        pltpu.VMEM((tiles, t, depth), BF16),
        pltpu.VMEM((lay.rows, depth), F32),
        pltpu.SemaphoreType.DMA((tiles,)),
        pltpu.SemaphoreType.DMA((len(pieces),)),
    ]
    body = functools.partial(down_body, lay, t, tiles, [len(c) for c in chunks])
    flops, moved = 2 * lay.rows * depth * width, 2 * depth * width
    return call(body, "down", [*pieces, wd], sum_outs(lay, depth), scratch, flops, moved)


def back_body(lay, t, split, count, *refs):
    pieces, wd_ref, refs = refs[:count], refs[count], refs[count + 1 :]
    outs = [refs[j * lay.h : (j + 1) * lay.h] for j in range(len(split))]
    refs = refs[len(split) * lay.h :]
    x_v, w_v, halves = refs[0], refs[1], refs[2 : 2 + lay.h]
    w_sem, in_sem, out_sem = refs[2 + lay.h :]
    small = start_all(load_rows([pieces], x_v, in_sem))
    loads = functools.partial(row_copies, t, wd_ref, w_v, w_sem)
    each(0, split[-1][1], lambda i: start_all(loads(i)) and None)
    wait_all(small)
    for (start, stop), group in zip(split, outs):

        def one(i, start=start, group=group):
            wait_all(loads(i))
            y = lax.dot_general(w_v[i], x_v[...], TRANSPOSED, preferred_element_type=F32)
            fill(lay, halves, i, y.T)
            start_all(store_copies(lay, t, start, halves, group, out_sem, i))

        each(start, stop, one)
    for (start, stop), group in zip(split, outs):
        each(
            start,
            stop,
            lambda i, start=start, group=group: wait_all(
                store_copies(lay, t, start, halves, group, out_sem, i)
            ),
        )


def pull_back(lay, pieces, wd, chunks):
    width, depth = wd.shape
    t = tile_of(width)
    tiles = width // t
    split = split_of(tiles, chunks)
    outs = []
    for start, stop in split:
        outs += half_outs(lay, (stop - start) * t)
    scratch = [
        pltpu.VMEM((lay.rows, depth), BF16),
        pltpu.VMEM((tiles, t, depth), BF16),
        *half_scratch(lay, tiles, t),
        pltpu.SemaphoreType.DMA((tiles,)),
        pltpu.SemaphoreType.DMA((len(pieces),)),
        pltpu.SemaphoreType.DMA((tiles, lay.h)),
    ]
    body = functools.partial(back_body, lay, t, split, len(pieces))
    flops, moved = 2 * lay.rows * depth * width, 2 * depth * width
    return grouped(
        lay, call(body, "back", [*pieces, wd], outs, scratch, flops, moved, direct=len(outs))
    )


def pull_body(lay, t, tiles, counts, *refs):
    chunks = []
    for n in counts:
        chunks.append(refs[:n])
        refs = refs[n:]
    tables, refs = refs[:4], refs[4:]
    outs = refs[: lay.cols]
    b_v, dests, acc, w_sem, in_sem = refs[lay.cols], refs[lay.cols + 1 : lay.cols + 5], *refs[-3:]
    small = start_all(load_rows(chunks, b_v, in_sem))
    loads = functools.partial(weight_copies, t, list(zip(tables, dests)), w_sem)
    each(0, tiles, lambda i: start_all(loads(i)) and None)
    acc[...] = jnp.zeros_like(acc)
    wait_all(small)
    wg_v, wu_v, s_v, a_v = dests
    shape = (lay.h, lay.q, lay.low, SUB, t)

    def one(i):
        wait_all(loads(i))
        back = b_v[:, cols_of(i, t)].astype(F32).reshape(shape)
        gp = (spread(lay, s_v[i]) * back).reshape(lay.rows, t).astype(BF16)
        up = (spread(lay, a_v[i]) * back).reshape(lay.rows, t).astype(BF16)
        acc[...] += lax.dot_general(
            wg_v[i], gp, TRANSPOSED, preferred_element_type=F32
        ) + lax.dot_general(wu_v[i], up, TRANSPOSED, preferred_element_type=F32)

    each(0, tiles, one)
    write_sum(lay, acc[...].T, outs)


def pull(lay, chunks, wg, wu, slope, act):
    depth, width = wg.shape
    t = tile_of(width)
    tiles = width // t
    pieces = [p for c in chunks for p in c]
    scratch = [
        pltpu.VMEM((lay.rows, width), BF16),
        pltpu.VMEM((tiles, depth, t), BF16),
        pltpu.VMEM((tiles, depth, t), BF16),
        pltpu.VMEM((tiles, lay.tokens, t), F32),
        pltpu.VMEM((tiles, lay.tokens, t), F32),
        pltpu.VMEM((depth, lay.rows), F32),
        pltpu.SemaphoreType.DMA((tiles, 4)),
        pltpu.SemaphoreType.DMA((len(pieces),)),
    ]
    body = functools.partial(pull_body, lay, t, tiles, [len(c) for c in chunks])
    flops, moved = 4 * lay.rows * depth * width, 4 * depth * width
    ins = [*pieces, wg, wu, slope, act]
    return call(body, "pull", ins, sum_outs(lay, depth), scratch, flops, moved)


def scatter_rows(lay, keep, sends):
    total = keep
    for k, s in enumerate(sends, 1):
        total = total + swap(s, "row", k).astype(F32)
    b = lay.block
    out = total[:b]
    for k in range(1, lay.q):
        out = out + swap(total[k * b : (k + 1) * b].astype(BF16), "row", k * lay.h).astype(F32)
    return out


def gather_rows(lay, own):
    near = [own] + [swap(own, "row", k * lay.h) for k in range(1, lay.q)]
    return near + [swap(p, "row", k) for k in range(1, lay.h) for p in near]


def scatter_cols(keep, sends):
    total = keep
    for k, s in enumerate(sends, 1):
        total = total + swap(s, "col", k).astype(F32)
    return total


def gather_cols(lay, own):
    return [own] + [swap(own, "col", k) for k in range(1, lay.cols)]


def token_sums(lay, gate, up, h):
    width = gate.shape[1]
    part = width // lay.h
    both = jnp.stack(
        [gate.reshape(lay.q, SUB, width), up.reshape(lay.q, SUB, width)], axis=1
    ).reshape(2 * lay.tokens, width)
    columns = lambda k: lax.dynamic_slice_in_dim(both, (h ^ k) * part, part, axis=1)
    total = columns(0)
    for k in range(1, lay.h):
        total = total + swap(columns(k), "row", k)
    b = 2 * SUB
    out = total[:b]
    for k in range(1, lay.q):
        out = out + swap(total[k * b : (k + 1) * b], "row", k * lay.h)
    own = out
    mine = jnp.concatenate([own] + [swap(own, "row", k * lay.h) for k in range(1, lay.q)], axis=0)
    full = jnp.zeros((2 * lay.tokens, width), F32)
    for k in range(lay.h):
        piece = mine if k == 0 else swap(mine, "row", k)
        full = lax.dynamic_update_slice_in_dim(full, piece, (h ^ k) * part, axis=1)
    full = full.reshape(lay.q, 2, SUB, width)
    return full[:, 0].reshape(lay.tokens, width), full[:, 1].reshape(lay.tokens, width)


def local(tokens, gain, gate_weight, up_weight, down_weight, probes):
    probe_count, token_count, depth = probes.shape
    lay = Layout(probe_count, token_count, lax.axis_size("row"), lax.axis_size("col"))
    r, c = lax.axis_index("row"), lax.axis_index("col")
    h, q = r % lay.h, r // lay.h
    blocks = probe_count * lay.q
    flip = (h * (lay.q * lay.low)) ^ (q * lay.low) ^ (c * (blocks // lay.cols))
    order = jnp.arange(blocks, dtype=jnp.int32) ^ flip
    token_order = jnp.arange(lay.q, dtype=jnp.int32) ^ ((flip // lay.low) % lay.q)
    five = (lay.h, lay.low, lay.q, SUB, depth)
    gain_row = gain[None, :]

    scaled = (tokens.astype(F32) * gain_row).astype(BF16)
    scaled = scaled.reshape(lay.q, SUB, depth)[token_order].reshape(token_count, depth)
    gate, up = token_sums(
        lay,
        jnp.dot(scaled, gate_weight, preferred_element_type=F32),
        jnp.dot(scaled, up_weight, preferred_element_type=F32),
        h,
    )
    sigmoid_gate = 1.0 / (1.0 + jnp.exp(-gate))
    act = gate * sigmoid_gate
    slope = sigmoid_gate * (1.0 + gate * (1.0 - sigmoid_gate)) * up

    natural = probes.reshape(five).transpose(0, 2, 1, 3, 4).reshape(blocks, SUB, depth)
    pushed = (natural[order].reshape(lay.rows, depth) * gain_row).astype(BF16)
    scale = levels = None
    entries = token_count * depth * lay.ranks
    for sweep in range(ITERS):
        chunks = []
        parts = push(lay, pushed, gate_weight, up_weight, slope, act, levels, CHUNKS)
        for k, (keep, *sends) in enumerate(parts):
            total = scatter_rows(lay, keep, sends)
            if levels is not None and k == 0:
                scale = lax.rsqrt(total[:, -128:-127] / entries + EPSILON)
                total = total[:, :-128]
            hidden = (total if scale is None else total * scale).astype(BF16)
            chunks.append(gather_rows(lay, hidden))
        res = down(lay, chunks, down_weight)
        tangent = scatter_cols(res[0], res[1:]).astype(BF16)
        tangents = gather_cols(lay, tangent)
        chunks = []
        for keep, *sends in pull_back(lay, tangents, down_weight, CHUNKS):
            back = scatter_rows(lay, keep, sends).astype(BF16)
            chunks.append(gather_rows(lay, back))
        res = pull(lay, chunks, gate_weight, up_weight, slope, act)
        pulled = scatter_cols(res[0], res[1:])
        final = sweep == ITERS - 1
        if final:
            grown = stack_rows(gather_cols(lay, pulled.astype(BF16))).astype(F32) * gain_row
        else:
            pushed = stack_rows(gather_cols(lay, (pulled * gain_row * gain_row).astype(BF16)))
            grown = pushed.astype(F32) / gain_row
        squares = jnp.sum(
            (grown * grown).reshape(lay.h, lay.q, lay.low, SUB, depth), axis=(1, 3, 4)
        )
        if final:
            outer = (flip // (lay.q * lay.low)) % lay.h
            inner = flip % lay.low
            far = (jnp.arange(lay.h) ^ outer)[:, None]
            near = (jnp.arange(lay.low) ^ inner)[None, :]
            level = lax.psum(squares[far, near].reshape(-1), "row") / entries
            basis = grown.reshape(blocks, SUB, depth)[order]
            basis = basis.reshape(lay.h, lay.q, lay.low, SUB, depth).transpose(0, 2, 1, 3, 4)
            basis = basis.reshape(probe_count, token_count, depth)
            return basis * lax.rsqrt(level + EPSILON)[:, None, None], jnp.sqrt(level)
        levels = jnp.broadcast_to(
            squares[:, None, :, None, None], (lay.h, lay.q, lay.low, SUB, 128)
        ).reshape(lay.rows, 128)


def solution(mesh):
    placed = (
        P(None, "row"),
        P("row"),
        P("row", "col"),
        P("row", "col"),
        P("col", "row"),
        P(None, None, "row"),
    )
    return jax.shard_map(
        local, mesh=mesh, in_specs=placed, out_specs=(P(None, None, "row"), P()), check_vma=False
    )
```

```python
import functools

import jax
import jax.numpy as jnp
from jax import lax
from jax.experimental import pallas as pl
from jax.experimental.pallas import tpu as pltpu
from jax.sharding import PartitionSpec as P

ITERS = 3
EPSILON = 1e-06
SUB = 8
CHUNKS = 2
F32 = jnp.float32
BF16 = jnp.bfloat16
TRANSPOSED = (((1,), (1,)), ((), ()))


def swap(x, axis, mask):
    n = lax.axis_size(axis)
    return lax.ppermute(x, axis, [(i, i ^ mask) for i in range(n)])


def stack_rows(pieces):
    if len(pieces) == 1:
        return pieces[0]
    if pieces[0].shape[0] % 16 == 0 or pieces[0].dtype == F32:
        return jnp.concatenate(pieces, axis=0)
    return jnp.concatenate([p.astype(F32) for p in pieces], axis=0).astype(pieces[0].dtype)


class Layout:
    def __init__(self, probes, tokens, ranks, cols):
        self.probes, self.tokens, self.ranks, self.cols = probes, tokens, ranks, cols
        self.rows = probes * tokens
        self.q = tokens // SUB
        self.h = ranks // self.q
        self.low = probes // self.h
        self.half = self.rows // self.h
        self.block = self.rows // ranks
        self.zrows = self.rows // cols

    def doubled(self):
        other = Layout(self.probes, self.tokens, self.ranks, self.cols)
        other.half, other.block = 2 * self.half, 2 * self.block
        return other


def any_spec():
    return pl.BlockSpec(memory_space=pl.ANY)


def call(body, name, ins, outs, scratch, flops, moved, direct=0):
    vmem = pl.BlockSpec(memory_space=pltpu.VMEM)
    return pl.pallas_call(
        body,
        in_specs=[any_spec()] * len(ins),
        out_specs=[any_spec()] * direct + [vmem] * (len(outs) - direct),
        out_shape=outs,
        scratch_shapes=scratch,
        compiler_params=pltpu.CompilerParams(vmem_limit_bytes=48 * 2**20),
        cost_estimate=pl.CostEstimate(flops=flops, bytes_accessed=moved, transcendentals=0),
        name=name,
    )(*ins)


def tile_of(extent):
    return max(t for t in range(128, 897, 128) if extent % t == 0)


def split_of(count, chunks):
    chunks = min(chunks, count)
    ends = [-(-count * (j + 1) // chunks) for j in range(chunks)]
    return list(zip([0] + ends[:-1], ends))


def spread(lay, per_token):
    return per_token.reshape(1, lay.q, 1, SUB, per_token.shape[-1])


def start_all(copies):
    for copy in copies:
        copy.start()
    return copies


def wait_all(copies):
    for copy in copies:
        copy.wait()


def load_rows(chunks, dest, sem):
    copies, col = [], 0
    for pieces in chunks:
        row, w = 0, pieces[0].shape[1]
        for p in pieces:
            n = p.shape[0]
            there = dest.at[pl.ds(row, n), pl.ds(col, w)]
            copies.append(pltpu.make_async_copy(p, there, sem.at[len(copies)]))
            row += n
        col += w
    return copies


def cols_of(i, t):
    return pl.ds(pl.multiple_of(i * t, t), t)


def each(start, stop, body):
    def step(i, carry):
        body(i)
        return carry

    lax.fori_loop(start, stop, step, 0)


def weight_copies(t, tables, sem, i):
    return [
        pltpu.make_async_copy(ref.at[:, cols_of(i, t)], dest.at[i], sem.at[i, k])
        for k, (ref, dest) in enumerate(tables)
    ]


def row_copies(t, ref, dest, sem, i):
    return [pltpu.make_async_copy(ref.at[cols_of(i, t), :], dest.at[i], sem.at[i])]


def store_copies(lay, t, start, halves, outs, sem, i):
    here = cols_of(i - start, t)
    return [
        pltpu.make_async_copy(v.at[i], o.at[:, here], sem.at[i, k])
        for k, (v, o) in enumerate(zip(halves, outs))
    ]


def fill(lay, halves, i, joined):
    for k, v in enumerate(halves):
        v[i] = joined[k * lay.half : (k + 1) * lay.half].astype(v.dtype)


def half_scratch(lay, tiles, t):
    return [pltpu.VMEM((tiles, lay.half, t), F32)] + [
        pltpu.VMEM((tiles, lay.half, t), BF16)
    ] * (lay.h - 1)


def push_body(lay, t, split, extra, *refs):
    x_ref, *tables = refs[:5]
    refs = refs[5:]
    sq_ref = refs[0] if extra else None
    refs = refs[extra:]
    outs = [refs[j * lay.h : (j + 1) * lay.h] for j in range(len(split))]
    refs = refs[len(split) * lay.h :]
    x_v, dests, sq_v, lev_v = refs[0], refs[1:5], refs[5], refs[6 : 6 + lay.h]
    halves = refs[6 + lay.h : 6 + 2 * lay.h]
    w_sem, in_sem, lev_sem, out_sem = refs[6 + 2 * lay.h :]
    count = split[-1][1]
    loads = functools.partial(weight_copies, t, list(zip(tables, dests)), w_sem)
    small = [pltpu.make_async_copy(x_ref, x_v, in_sem.at[0])]
    if extra:
        small.append(pltpu.make_async_copy(sq_ref, sq_v, in_sem.at[1]))
    start_all(small)
    each(0, count, lambda i: start_all(loads(i)) and None)
    wait_all(small)
    tail = []
    if extra:
        w = (split[0][1] - split[0][0]) * t
        for k, v in enumerate(lev_v):
            v[...] = sq_v[k * lay.half : (k + 1) * lay.half, :].astype(v.dtype)
            there = outs[0][k].at[:, pl.ds(w, 128)]
            tail.append(pltpu.make_async_copy(v, there, lev_sem.at[k]))
        start_all(tail)
    for (start, stop), group in zip(split, outs):

        def one(i, start=start, group=group):
            wait_all(loads(i))
            x = x_v[...]
            wg_v, wu_v, s_v, a_v = dests
            g = jnp.dot(x, wg_v[i], preferred_element_type=F32)
            u = jnp.dot(x, wu_v[i], preferred_element_type=F32)
            shape = (lay.h, lay.q, lay.low, SUB, t)
            s, a = spread(lay, s_v[i]), spread(lay, a_v[i])
            fill(lay, halves, i, (s * g.reshape(shape) + a * u.reshape(shape)).reshape(lay.rows, t))
            start_all(store_copies(lay, t, start, halves, group, out_sem, i))

        each(start, stop, one)
    for (start, stop), group in zip(split, outs):
        each(
            start,
            stop,
            lambda i, start=start, group=group: wait_all(
                store_copies(lay, t, start, halves, group, out_sem, i)
            ),
        )
    wait_all(tail)


def half_outs(lay, w):
    return [jax.ShapeDtypeStruct((lay.half, w), F32)] + [
        jax.ShapeDtypeStruct((lay.half, w), BF16)
    ] * (lay.h - 1)


def grouped(lay, outs):
    return [outs[j : j + lay.h] for j in range(0, len(outs), lay.h)]


def push(lay, x, wg, wu, slope, act, squares, chunks):
    depth, width = wg.shape
    t = tile_of(width)
    tiles = width // t
    split = split_of(tiles, chunks)
    extra = squares is not None
    outs = []
    for j, (start, stop) in enumerate(split):
        outs += half_outs(lay, (stop - start) * t + (128 if extra and j == 0 else 0))
    scratch = [
        pltpu.VMEM(x.shape, BF16),
        pltpu.VMEM((tiles, depth, t), BF16),
        pltpu.VMEM((tiles, depth, t), BF16),
        pltpu.VMEM((tiles, lay.tokens, t), F32),
        pltpu.VMEM((tiles, lay.tokens, t), F32),
        pltpu.VMEM((lay.rows, 128), F32),
        *[pltpu.VMEM((lay.half, 128), o.dtype) for o in outs[: lay.h]],
        *half_scratch(lay, tiles, t),
        pltpu.SemaphoreType.DMA((tiles, 4)),
        pltpu.SemaphoreType.DMA((2,)),
        pltpu.SemaphoreType.DMA((lay.h,)),
        pltpu.SemaphoreType.DMA((tiles, lay.h)),
    ]
    ins = [x, wg, wu, slope, act] + ([squares] if extra else [])
    body = functools.partial(push_body, lay, t, split, int(extra))
    flops, moved = 4 * lay.rows * depth * width, 4 * depth * width
    return grouped(lay, call(body, "push", ins, outs, scratch, flops, moved, direct=len(outs)))


def first_body(lay, twin, t, split, *refs):
    xt_ref, xp_ref, wg_ref, wu_ref, tok_out = refs[:5]
    refs = refs[5:]
    outs = [refs[j * lay.h : (j + 1) * lay.h] for j in range(len(split))]
    refs = refs[len(split) * lay.h :]
    x_v, wg_v, wu_v, tok_v, halves = *refs[:4], refs[4 : 4 + lay.h]
    w_sem, in_sem, tok_sem, out_sem = refs[4 + lay.h :]
    count, n = split[-1][1], lay.tokens
    loads = functools.partial(weight_copies, t, [(wg_ref, wg_v), (wu_ref, wu_v)], w_sem)
    small = start_all(
        [
            pltpu.make_async_copy(xt_ref, x_v.at[pl.ds(0, n)], in_sem.at[0]),
            pltpu.make_async_copy(xp_ref, x_v.at[pl.ds(n, lay.rows)], in_sem.at[1]),
        ]
    )
    each(0, count, lambda i: start_all(loads(i)) and None)
    wait_all(small)

    def stores(i, start, group):
        token = pltpu.make_async_copy(tok_v.at[i], tok_out.at[:, cols_of(i, t)], tok_sem.at[i])
        return [token] + store_copies(twin, t, start, halves, group, out_sem, i)

    for (start, stop), group in zip(split, outs):

        def one(i, start=start, group=group):
            wait_all(loads(i))
            x = x_v[...]
            g = jnp.dot(x, wg_v[i], preferred_element_type=F32)
            u = jnp.dot(x, wu_v[i], preferred_element_type=F32)
            shape = (lay.q, 1, SUB, t)
            both = jnp.concatenate([g[:n].reshape(shape), u[:n].reshape(shape)], axis=1)
            tok_v[i] = both.reshape(2 * n, t)
            shape = (lay.ranks, 1, lay.block, t)
            raw = jnp.concatenate([g[n:].reshape(shape), u[n:].reshape(shape)], axis=1)
            fill(twin, halves, i, raw.reshape(2 * lay.rows, t))
            start_all(stores(i, start, group))

        each(start, stop, one)
    for (start, stop), group in zip(split, outs):
        each(start, stop, lambda i, start=start, group=group: wait_all(stores(i, start, group)))


def first(lay, tokens, x, wg, wu, chunks):
    depth, width = wg.shape
    twin = lay.doubled()
    t = tile_of(width)
    tiles = width // t
    split = split_of(tiles, chunks)
    outs = [jax.ShapeDtypeStruct((2 * lay.tokens, width), F32)]
    for start, stop in split:
        outs += half_outs(twin, (stop - start) * t)
    rows = lay.tokens + lay.rows
    scratch = [
        pltpu.VMEM((rows, depth), BF16),
        pltpu.VMEM((tiles, depth, t), BF16),
        pltpu.VMEM((tiles, depth, t), BF16),
        pltpu.VMEM((tiles, 2 * lay.tokens, t), F32),
        *half_scratch(twin, tiles, t),
        pltpu.SemaphoreType.DMA((tiles, 2)),
        pltpu.SemaphoreType.DMA((2,)),
        pltpu.SemaphoreType.DMA((tiles,)),
        pltpu.SemaphoreType.DMA((tiles, lay.h)),
    ]
    body = functools.partial(first_body, lay, twin, t, split)
    flops, moved = 4 * rows * depth * width, 4 * depth * width
    ins = [tokens, x, wg, wu]
    tok, *rest = call(body, "first", ins, outs, scratch, flops, moved, direct=len(outs))
    return tok, grouped(lay, rest)


def write_sum(lay, total, outs):
    outs[0][...] = total[: lay.zrows]
    for k, ref in enumerate(outs[1:], 1):
        ref[...] = total[k * lay.zrows : (k + 1) * lay.zrows].astype(BF16)


def sum_outs(lay, depth):
    return [jax.ShapeDtypeStruct((lay.zrows, depth), F32)] + [
        jax.ShapeDtypeStruct((lay.zrows, depth), BF16)
    ] * (lay.cols - 1)


def down_body(lay, t, tiles, counts, *refs):
    chunks = []
    for n in counts:
        chunks.append(refs[:n])
        refs = refs[n:]
    wd_ref, refs = refs[0], refs[1:]
    outs = refs[: lay.cols]
    x_v, w_v, acc, w_sem, in_sem = refs[lay.cols :]
    small = start_all(load_rows(chunks, x_v, in_sem))
    loads = functools.partial(row_copies, t, wd_ref, w_v, w_sem)
    each(0, tiles, lambda i: start_all(loads(i)) and None)
    acc[...] = jnp.zeros_like(acc)
    wait_all(small)

    def one(i):
        wait_all(loads(i))
        acc[...] += jnp.dot(x_v[:, cols_of(i, t)], w_v[i], preferred_element_type=F32)

    each(0, tiles, one)
    write_sum(lay, acc[...], outs)


def down(lay, chunks, wd):
    width, depth = wd.shape
    t = tile_of(width)
    tiles = width // t
    pieces = [p for c in chunks for p in c]
    scratch = [
        pltpu.VMEM((lay.rows, width), BF16),
        pltpu.VMEM((tiles, t, depth), BF16),
        pltpu.VMEM((lay.rows, depth), F32),
        pltpu.SemaphoreType.DMA((tiles,)),
        pltpu.SemaphoreType.DMA((len(pieces),)),
    ]
    body = functools.partial(down_body, lay, t, tiles, [len(c) for c in chunks])
    flops, moved = 2 * lay.rows * depth * width, 2 * depth * width
    return call(body, "down", [*pieces, wd], sum_outs(lay, depth), scratch, flops, moved)


def back_body(lay, t, split, count, *refs):
    pieces, wd_ref, refs = refs[:count], refs[count], refs[count + 1 :]
    outs = [refs[j * lay.h : (j + 1) * lay.h] for j in range(len(split))]
    refs = refs[len(split) * lay.h :]
    x_v, w_v, halves = refs[0], refs[1], refs[2 : 2 + lay.h]
    w_sem, in_sem, out_sem = refs[2 + lay.h :]
    small = start_all(load_rows([pieces], x_v, in_sem))
    loads = functools.partial(row_copies, t, wd_ref, w_v, w_sem)
    each(0, split[-1][1], lambda i: start_all(loads(i)) and None)
    wait_all(small)
    for (start, stop), group in zip(split, outs):

        def one(i, start=start, group=group):
            wait_all(loads(i))
            y = lax.dot_general(w_v[i], x_v[...], TRANSPOSED, preferred_element_type=F32)
            fill(lay, halves, i, y.T)
            start_all(store_copies(lay, t, start, halves, group, out_sem, i))

        each(start, stop, one)
    for (start, stop), group in zip(split, outs):
        each(
            start,
            stop,
            lambda i, start=start, group=group: wait_all(
                store_copies(lay, t, start, halves, group, out_sem, i)
            ),
        )


def pull_back(lay, pieces, wd, chunks):
    width, depth = wd.shape
    t = tile_of(width)
    tiles = width // t
    split = split_of(tiles, chunks)
    outs = []
    for start, stop in split:
        outs += half_outs(lay, (stop - start) * t)
    scratch = [
        pltpu.VMEM((lay.rows, depth), BF16),
        pltpu.VMEM((tiles, t, depth), BF16),
        *half_scratch(lay, tiles, t),
        pltpu.SemaphoreType.DMA((tiles,)),
        pltpu.SemaphoreType.DMA((len(pieces),)),
        pltpu.SemaphoreType.DMA((tiles, lay.h)),
    ]
    body = functools.partial(back_body, lay, t, split, len(pieces))
    flops, moved = 2 * lay.rows * depth * width, 2 * depth * width
    return grouped(
        lay, call(body, "back", [*pieces, wd], outs, scratch, flops, moved, direct=len(outs))
    )


def pull_body(lay, t, tiles, counts, *refs):
    chunks = []
    for n in counts:
        chunks.append(refs[:n])
        refs = refs[n:]
    tables, refs = refs[:4], refs[4:]
    outs = refs[: lay.cols]
    b_v, dests, acc, w_sem, in_sem = refs[lay.cols], refs[lay.cols + 1 : lay.cols + 5], *refs[-3:]
    small = start_all(load_rows(chunks, b_v, in_sem))
    loads = functools.partial(weight_copies, t, list(zip(tables, dests)), w_sem)
    each(0, tiles, lambda i: start_all(loads(i)) and None)
    acc[...] = jnp.zeros_like(acc)
    wait_all(small)
    wg_v, wu_v, s_v, a_v = dests
    shape = (lay.h, lay.q, lay.low, SUB, t)

    def one(i):
        wait_all(loads(i))
        back = b_v[:, cols_of(i, t)].astype(F32).reshape(shape)
        gp = (spread(lay, s_v[i]) * back).reshape(lay.rows, t).astype(BF16)
        up = (spread(lay, a_v[i]) * back).reshape(lay.rows, t).astype(BF16)
        acc[...] += lax.dot_general(
            wg_v[i], gp, TRANSPOSED, preferred_element_type=F32
        ) + lax.dot_general(wu_v[i], up, TRANSPOSED, preferred_element_type=F32)

    each(0, tiles, one)
    write_sum(lay, acc[...].T, outs)


def pull(lay, chunks, wg, wu, slope, act):
    depth, width = wg.shape
    t = tile_of(width)
    tiles = width // t
    pieces = [p for c in chunks for p in c]
    scratch = [
        pltpu.VMEM((lay.rows, width), BF16),
        pltpu.VMEM((tiles, depth, t), BF16),
        pltpu.VMEM((tiles, depth, t), BF16),
        pltpu.VMEM((tiles, lay.tokens, t), F32),
        pltpu.VMEM((tiles, lay.tokens, t), F32),
        pltpu.VMEM((depth, lay.rows), F32),
        pltpu.SemaphoreType.DMA((tiles, 4)),
        pltpu.SemaphoreType.DMA((len(pieces),)),
    ]
    body = functools.partial(pull_body, lay, t, tiles, [len(c) for c in chunks])
    flops, moved = 4 * lay.rows * depth * width, 4 * depth * width
    ins = [*pieces, wg, wu, slope, act]
    return call(body, "pull", ins, sum_outs(lay, depth), scratch, flops, moved)


def scatter_rows(lay, keep, sends):
    total = keep
    for k, s in enumerate(sends, 1):
        total = total + swap(s, "row", k).astype(F32)
    b = lay.block
    out = total[:b]
    for k in range(1, lay.q):
        out = out + swap(total[k * b : (k + 1) * b].astype(BF16), "row", k * lay.h).astype(F32)
    return out


def gather_rows(lay, own):
    near = [own] + [swap(own, "row", k * lay.h) for k in range(1, lay.q)]
    far = jnp.concatenate(near[1:], axis=0)
    return near + [swap(p, "row", k) for k in range(1, lay.h) for p in (own, far)]


def scatter_cols(keep, sends):
    total = keep
    for k, s in enumerate(sends, 1):
        total = total + swap(s, "col", k).astype(F32)
    return total


def gather_cols(lay, own):
    return [own] + [swap(own, "col", k) for k in range(1, lay.cols)]


def scatter_tokens(lay, both, h):
    part = both.shape[1] // lay.h
    columns = lambda k: lax.dynamic_slice_in_dim(both, (h ^ k) * part, part, axis=1)
    total = columns(0)
    for k in range(1, lay.h):
        total = total + swap(columns(k), "row", k)
    b = 2 * SUB
    out = total[:b]
    for k in range(1, lay.q):
        out = out + swap(total[k * b : (k + 1) * b], "row", k * lay.h)
    return out


def join_columns(lay, mine, h):
    part = mine.shape[1]
    full = jnp.zeros((mine.shape[0], part * lay.h), mine.dtype)
    for k in range(lay.h):
        piece = mine if k == 0 else swap(mine, "row", k)
        full = lax.dynamic_update_slice_in_dim(full, piece, (h ^ k) * part, axis=1)
    return full


def gates_of(joined):
    both = joined.reshape(-1, 2, SUB, joined.shape[1])
    rows = both.shape[0] * SUB
    gate, up = both[:, 0].reshape(rows, -1), both[:, 1].reshape(rows, -1)
    sigmoid_gate = 1.0 / (1.0 + jnp.exp(-gate))
    act = gate * sigmoid_gate
    return sigmoid_gate * (1.0 + gate * (1.0 - sigmoid_gate)) * up, act


def local(tokens, gain, gate_weight, up_weight, down_weight, probes):
    probe_count, token_count, depth = probes.shape
    lay = Layout(probe_count, token_count, lax.axis_size("row"), lax.axis_size("col"))
    r, c = lax.axis_index("row"), lax.axis_index("col")
    h, q = r % lay.h, r // lay.h
    blocks = probe_count * lay.q
    flip = (h * (lay.q * lay.low)) ^ (q * lay.low) ^ (c * (blocks // lay.cols))
    order = jnp.arange(blocks, dtype=jnp.int32) ^ flip
    token_order = jnp.arange(lay.q, dtype=jnp.int32) ^ ((flip // lay.low) % lay.q)
    five = (lay.h, lay.low, lay.q, SUB, depth)
    gain_row = gain[None, :]

    scaled = (tokens.astype(F32) * gain_row).astype(BF16)
    scaled = scaled.reshape(lay.q, SUB, depth)[token_order].reshape(token_count, depth)
    natural = probes.reshape(five).transpose(0, 2, 1, 3, 4).reshape(blocks, SUB, depth)
    pushed = (natural[order].reshape(lay.rows, depth) * gain_row).astype(BF16)
    tok, parts = first(lay, scaled, pushed, gate_weight, up_weight, CHUNKS)
    own = scatter_tokens(lay, tok, h)
    own_slope, own_act = gates_of(join_columns(lay, own, h))
    own_slope = jnp.tile(own_slope, (lay.low, 1))
    own_act = jnp.tile(own_act, (lay.low, 1))
    levels = None
    entries = token_count * depth * lay.ranks
    for sweep in range(ITERS):
        chunks = []
        if sweep:
            parts = push(lay, pushed, gate_weight, up_weight, slope, act, levels, CHUNKS)
        at = 0
        for k, (keep, *sends) in enumerate(parts):
            if sweep == 0:
                total = scatter_rows(lay.doubled(), keep, sends)
                here = slice(at, at + total.shape[1])
                at += total.shape[1]
                total = own_slope[:, here] * total[: lay.block] + own_act[:, here] * total[lay.block :]
            else:
                total = scatter_rows(lay, keep, sends)
                if k == 0:
                    scale = lax.rsqrt(total[:, -128:-127] / entries + EPSILON)
                    total = total[:, :-128]
                total = total * scale
            chunks.append(gather_rows(lay, total.astype(BF16)))
        res = down(lay, chunks, down_weight)
        tangent = scatter_cols(res[0], res[1:]).astype(BF16)
        if sweep == 0:
            tangent, own = lax.optimization_barrier((tangent, own))
            mine = [own] + [swap(own, "row", k * lay.h) for k in range(1, lay.q)]
            slope, act = gates_of(join_columns(lay, jnp.concatenate(mine, axis=0), h))
        tangents = gather_cols(lay, tangent)
        chunks = []
        for keep, *sends in pull_back(lay, tangents, down_weight, CHUNKS):
            back = scatter_rows(lay, keep, sends).astype(BF16)
            chunks.append(gather_rows(lay, back))
        res = pull(lay, chunks, gate_weight, up_weight, slope, act)
        pulled = scatter_cols(res[0], res[1:])
        final = sweep == ITERS - 1
        if final:
            grown = stack_rows(gather_cols(lay, pulled.astype(BF16))).astype(F32) * gain_row
        else:
            pushed = stack_rows(gather_cols(lay, (pulled * gain_row * gain_row).astype(BF16)))
            grown = pushed.astype(F32) / gain_row
        squares = jnp.sum(
            (grown * grown).reshape(lay.h, lay.q, lay.low, SUB, depth), axis=(1, 3, 4)
        )
        if final:
            outer = (flip // (lay.q * lay.low)) % lay.h
            inner = flip % lay.low
            far = (jnp.arange(lay.h) ^ outer)[:, None]
            near = (jnp.arange(lay.low) ^ inner)[None, :]
            level = squares[far, near].reshape(-1)
            mask = 1
            while mask < lay.ranks:
                level = level + swap(level, "row", mask)
                mask *= 2
            level = level / entries
            basis = grown.reshape(blocks, SUB, depth)[order]
            basis = basis.reshape(lay.h, lay.q, lay.low, SUB, depth).transpose(0, 2, 1, 3, 4)
            basis = basis.reshape(probe_count, token_count, depth)
            return basis * lax.rsqrt(level + EPSILON)[:, None, None], jnp.sqrt(level)
        levels = jnp.broadcast_to(
            squares[:, None, :, None, None], (lay.h, lay.q, lay.low, SUB, 128)
        ).reshape(lay.rows, 128)


def solution(mesh):
    placed = (
        P(None, "row"),
        P("row"),
        P("row", "col"),
        P("row", "col"),
        P("col", "row"),
        P(None, None, "row"),
    )
    return jax.shard_map(
        local, mesh=mesh, in_specs=placed, out_specs=(P(None, None, "row"), P()), check_vma=False
    )
```

```python
import functools

import jax
import jax.numpy as jnp
from jax import lax
from jax.experimental import pallas as pl
from jax.experimental.pallas import tpu as pltpu
from jax.sharding import PartitionSpec as P


ITERS = 3
EPSILON = 1e-06
SUB = 8
CHUNKS = 2
F32 = jnp.float32
BF16 = jnp.bfloat16
TRANSPOSED = (((1,), (1,)), ((), ()))


def swap(x, axis, mask):
    n = lax.axis_size(axis)
    return lax.ppermute(x, axis, [(i, i ^ mask) for i in range(n)])


def stack_rows(pieces):
    if len(pieces) == 1:
        return pieces[0]
    if pieces[0].shape[0] % 16 == 0 or pieces[0].dtype == F32:
        return jnp.concatenate(pieces, axis=0)
    return jnp.concatenate([p.astype(F32) for p in pieces], axis=0).astype(pieces[0].dtype)


class Layout:
    def __init__(self, probes, tokens, ranks, cols):
        self.probes, self.tokens, self.ranks, self.cols = probes, tokens, ranks, cols
        self.rows = probes * tokens
        self.q = tokens // SUB
        self.h = ranks // self.q
        self.low = probes // self.h
        self.half = self.rows // self.h
        self.block = self.rows // ranks
        self.zrows = self.rows // cols

    def doubled(self):
        other = Layout(self.probes, self.tokens, self.ranks, self.cols)
        other.half, other.block = 2 * self.half, 2 * self.block
        return other


def any_spec():
    return pl.BlockSpec(memory_space=pl.ANY)


def call(body, ins, outs, scratch, flops, moved, direct=0):
    vmem = pl.BlockSpec(memory_space=pltpu.VMEM)
    return pl.pallas_call(
        body,
        in_specs=[any_spec()] * len(ins),
        out_specs=[any_spec()] * direct + [vmem] * (len(outs) - direct),
        out_shape=outs,
        scratch_shapes=scratch,
        compiler_params=pltpu.CompilerParams(vmem_limit_bytes=48 * 2**20),
        cost_estimate=pl.CostEstimate(flops=flops, bytes_accessed=moved, transcendentals=0),
    )(*ins)


def tile_of(extent):
    return max(t for t in range(128, 897, 128) if extent % t == 0)


def split_of(count, chunks):
    chunks = min(chunks, count)
    ends = [-(-count * (j + 1) // chunks) for j in range(chunks)]
    return list(zip([0] + ends[:-1], ends))


def spread(lay, per_token):
    return per_token.reshape(1, lay.q, 1, SUB, per_token.shape[-1])


def start_all(copies):
    for copy in copies:
        copy.start()
    return copies


def wait_all(copies):
    for copy in copies:
        copy.wait()


def load_rows(chunks, dest, sem):
    copies, col = [], 0
    for pieces in chunks:
        row, w = 0, pieces[0].shape[1]
        for p in pieces:
            n = p.shape[0]
            there = dest.at[pl.ds(row, n), pl.ds(col, w)]
            copies.append(pltpu.make_async_copy(p, there, sem.at[len(copies)]))
            row += n
        col += w
    return copies


def cols_of(i, t):
    return pl.ds(pl.multiple_of(i * t, t), t)


def each(start, stop, body):
    def step(i, carry):
        body(i)
        return carry

    lax.fori_loop(start, stop, step, 0)


def weight_copies(t, tables, sem, i):
    return [
        pltpu.make_async_copy(ref.at[:, cols_of(i, t)], dest.at[i], sem.at[i, k])
        for k, (ref, dest) in enumerate(tables)
    ]


def row_copies(t, ref, dest, sem, i):
    return [pltpu.make_async_copy(ref.at[cols_of(i, t), :], dest.at[i], sem.at[i])]


def store_copies(t, start, halves, outs, sem, i):
    here = cols_of(i - start, t)
    return [
        pltpu.make_async_copy(v.at[i], o.at[:, here], sem.at[i, k])
        for k, (v, o) in enumerate(zip(halves, outs))
    ]


def fill(lay, halves, i, joined):
    for k, v in enumerate(halves):
        v[i] = joined[k * lay.half : (k + 1) * lay.half].astype(v.dtype)


def half_scratch(lay, tiles, t):
    return [pltpu.VMEM((tiles, lay.half, t), F32)] + [
        pltpu.VMEM((tiles, lay.half, t), BF16)
    ] * (lay.h - 1)


def push_body(lay, t, split, extra, *refs):
    x_ref, *tables = refs[:5]
    refs = refs[5:]
    sq_ref = refs[0] if extra else None
    refs = refs[extra:]
    outs = [refs[j * lay.h : (j + 1) * lay.h] for j in range(len(split))]
    refs = refs[len(split) * lay.h :]
    x_v, dests, sq_v, lev_v = refs[0], refs[1:5], refs[5], refs[6 : 6 + lay.h]
    halves = refs[6 + lay.h : 6 + 2 * lay.h]
    w_sem, in_sem, lev_sem, out_sem = refs[6 + 2 * lay.h :]
    count = split[-1][1]
    loads = functools.partial(weight_copies, t, list(zip(tables, dests)), w_sem)
    small = [pltpu.make_async_copy(x_ref, x_v, in_sem.at[0])]
    if extra:
        small.append(pltpu.make_async_copy(sq_ref, sq_v, in_sem.at[1]))
    start_all(small)
    each(0, count, lambda i: start_all(loads(i)) and None)
    wait_all(small)
    tail = []
    if extra:
        w = (split[0][1] - split[0][0]) * t
        for k, v in enumerate(lev_v):
            v[...] = sq_v[k * lay.half : (k + 1) * lay.half, :].astype(v.dtype)
            there = outs[0][k].at[:, pl.ds(w, 128)]
            tail.append(pltpu.make_async_copy(v, there, lev_sem.at[k]))
        start_all(tail)
    for (start, stop), group in zip(split, outs):

        def one(i, start=start, group=group):
            wait_all(loads(i))
            x = x_v[...]
            wg_v, wu_v, s_v, a_v = dests
            g = jnp.dot(x, wg_v[i], preferred_element_type=F32)
            u = jnp.dot(x, wu_v[i], preferred_element_type=F32)
            shape = (lay.h, lay.q, lay.low, SUB, t)
            s, a = spread(lay, s_v[i]), spread(lay, a_v[i])
            fill(lay, halves, i, (s * g.reshape(shape) + a * u.reshape(shape)).reshape(lay.rows, t))
            start_all(store_copies(t, start, halves, group, out_sem, i))

        each(start, stop, one)
    for (start, stop), group in zip(split, outs):
        each(
            start,
            stop,
            lambda i, start=start, group=group: wait_all(
                store_copies(t, start, halves, group, out_sem, i)
            ),
        )
    wait_all(tail)


def half_outs(lay, w):
    return [jax.ShapeDtypeStruct((lay.half, w), F32)] + [
        jax.ShapeDtypeStruct((lay.half, w), BF16)
    ] * (lay.h - 1)


def grouped(lay, outs):
    return [outs[j : j + lay.h] for j in range(0, len(outs), lay.h)]


def push(lay, x, wg, wu, slope, act, squares, chunks):
    depth, width = wg.shape
    t = tile_of(width)
    tiles = width // t
    split = split_of(tiles, chunks)
    extra = squares is not None
    outs = []
    for j, (start, stop) in enumerate(split):
        outs += half_outs(lay, (stop - start) * t + (128 if extra and j == 0 else 0))
    scratch = [
        pltpu.VMEM(x.shape, BF16),
        pltpu.VMEM((tiles, depth, t), BF16),
        pltpu.VMEM((tiles, depth, t), BF16),
        pltpu.VMEM((tiles, lay.tokens, t), F32),
        pltpu.VMEM((tiles, lay.tokens, t), F32),
        pltpu.VMEM((lay.rows, 128), F32),
        *[pltpu.VMEM((lay.half, 128), o.dtype) for o in outs[: lay.h]],
        *half_scratch(lay, tiles, t),
        pltpu.SemaphoreType.DMA((tiles, 4)),
        pltpu.SemaphoreType.DMA((2,)),
        pltpu.SemaphoreType.DMA((lay.h,)),
        pltpu.SemaphoreType.DMA((tiles, lay.h)),
    ]
    ins = [x, wg, wu, slope, act] + ([squares] if extra else [])
    body = functools.partial(push_body, lay, t, split, int(extra))
    flops, moved = 4 * lay.rows * depth * width, 4 * depth * width
    return grouped(lay, call(body, ins, outs, scratch, flops, moved, direct=len(outs)))


def first_body(lay, twin, t, split, *refs):
    xt_ref, xp_ref, wg_ref, wu_ref, tok_out = refs[:5]
    refs = refs[5:]
    outs = [refs[j * lay.h : (j + 1) * lay.h] for j in range(len(split))]
    refs = refs[len(split) * lay.h :]
    x_v, wg_v, wu_v, tok_v, halves = *refs[:4], refs[4 : 4 + lay.h]
    w_sem, in_sem, tok_sem, out_sem = refs[4 + lay.h :]
    count, n = split[-1][1], lay.tokens
    loads = functools.partial(weight_copies, t, [(wg_ref, wg_v), (wu_ref, wu_v)], w_sem)
    small = start_all(
        [
            pltpu.make_async_copy(xt_ref, x_v.at[pl.ds(0, n)], in_sem.at[0]),
            pltpu.make_async_copy(xp_ref, x_v.at[pl.ds(n, lay.rows)], in_sem.at[1]),
        ]
    )
    each(0, count, lambda i: start_all(loads(i)) and None)
    wait_all(small)

    def stores(i, start, group):
        token = pltpu.make_async_copy(tok_v.at[i], tok_out.at[:, cols_of(i, t)], tok_sem.at[i])
        return [token] + store_copies(t, start, halves, group, out_sem, i)

    for (start, stop), group in zip(split, outs):

        def one(i, start=start, group=group):
            wait_all(loads(i))
            x = x_v[...]
            g = jnp.dot(x, wg_v[i], preferred_element_type=F32)
            u = jnp.dot(x, wu_v[i], preferred_element_type=F32)
            shape = (lay.q, 1, SUB, t)
            both = jnp.concatenate([g[:n].reshape(shape), u[:n].reshape(shape)], axis=1)
            tok_v[i] = both.reshape(2 * n, t)
            shape = (lay.ranks, 1, lay.block, t)
            raw = jnp.concatenate([g[n:].reshape(shape), u[n:].reshape(shape)], axis=1)
            fill(twin, halves, i, raw.reshape(2 * lay.rows, t))
            start_all(stores(i, start, group))

        each(start, stop, one)
    for (start, stop), group in zip(split, outs):
        each(start, stop, lambda i, start=start, group=group: wait_all(stores(i, start, group)))


def first(lay, tokens, x, wg, wu, chunks):
    depth, width = wg.shape
    twin = lay.doubled()
    t = tile_of(width)
    tiles = width // t
    split = split_of(tiles, chunks)
    outs = [jax.ShapeDtypeStruct((2 * lay.tokens, width), F32)]
    for start, stop in split:
        outs += half_outs(twin, (stop - start) * t)
    rows = lay.tokens + lay.rows
    scratch = [
        pltpu.VMEM((rows, depth), BF16),
        pltpu.VMEM((tiles, depth, t), BF16),
        pltpu.VMEM((tiles, depth, t), BF16),
        pltpu.VMEM((tiles, 2 * lay.tokens, t), F32),
        *half_scratch(twin, tiles, t),
        pltpu.SemaphoreType.DMA((tiles, 2)),
        pltpu.SemaphoreType.DMA((2,)),
        pltpu.SemaphoreType.DMA((tiles,)),
        pltpu.SemaphoreType.DMA((tiles, lay.h)),
    ]
    body = functools.partial(first_body, lay, twin, t, split)
    flops, moved = 4 * rows * depth * width, 4 * depth * width
    ins = [tokens, x, wg, wu]
    tok, *rest = call(body, ins, outs, scratch, flops, moved, direct=len(outs))
    return tok, grouped(lay, rest)


def write_sum(lay, total, outs):
    outs[0][...] = total[: lay.zrows]
    for k, ref in enumerate(outs[1:], 1):
        ref[...] = total[k * lay.zrows : (k + 1) * lay.zrows].astype(BF16)


def sum_outs(lay, depth):
    return [jax.ShapeDtypeStruct((lay.zrows, depth), F32)] + [
        jax.ShapeDtypeStruct((lay.zrows, depth), BF16)
    ] * (lay.cols - 1)


def down_body(lay, t, tiles, counts, *refs):
    chunks = []
    for n in counts:
        chunks.append(refs[:n])
        refs = refs[n:]
    wd_ref, refs = refs[0], refs[1:]
    outs = refs[: lay.cols]
    x_v, w_v, acc, w_sem, in_sem = refs[lay.cols :]
    small = start_all(load_rows(chunks, x_v, in_sem))
    loads = functools.partial(row_copies, t, wd_ref, w_v, w_sem)
    each(0, tiles, lambda i: start_all(loads(i)) and None)
    acc[...] = jnp.zeros_like(acc)
    wait_all(small)

    def one(i):
        wait_all(loads(i))
        acc[...] += jnp.dot(x_v[:, cols_of(i, t)], w_v[i], preferred_element_type=F32)

    each(0, tiles, one)
    write_sum(lay, acc[...], outs)


def down(lay, chunks, wd):
    width, depth = wd.shape
    t = tile_of(width)
    tiles = width // t
    pieces = [p for c in chunks for p in c]
    scratch = [
        pltpu.VMEM((lay.rows, width), BF16),
        pltpu.VMEM((tiles, t, depth), BF16),
        pltpu.VMEM((lay.rows, depth), F32),
        pltpu.SemaphoreType.DMA((tiles,)),
        pltpu.SemaphoreType.DMA((len(pieces),)),
    ]
    body = functools.partial(down_body, lay, t, tiles, [len(c) for c in chunks])
    flops, moved = 2 * lay.rows * depth * width, 2 * depth * width
    return call(body, [*pieces, wd], sum_outs(lay, depth), scratch, flops, moved)


def back_body(lay, t, split, count, *refs):
    pieces, wd_ref, refs = refs[:count], refs[count], refs[count + 1 :]
    outs = [refs[j * lay.h : (j + 1) * lay.h] for j in range(len(split))]
    refs = refs[len(split) * lay.h :]
    x_v, w_v, halves = refs[0], refs[1], refs[2 : 2 + lay.h]
    w_sem, in_sem, out_sem = refs[2 + lay.h :]
    small = start_all(load_rows([pieces], x_v, in_sem))
    loads = functools.partial(row_copies, t, wd_ref, w_v, w_sem)
    each(0, split[-1][1], lambda i: start_all(loads(i)) and None)
    wait_all(small)
    for (start, stop), group in zip(split, outs):

        def one(i, start=start, group=group):
            wait_all(loads(i))
            y = lax.dot_general(w_v[i], x_v[...], TRANSPOSED, preferred_element_type=F32)
            fill(lay, halves, i, y.T)
            start_all(store_copies(t, start, halves, group, out_sem, i))

        each(start, stop, one)
    for (start, stop), group in zip(split, outs):
        each(
            start,
            stop,
            lambda i, start=start, group=group: wait_all(
                store_copies(t, start, halves, group, out_sem, i)
            ),
        )


def pull_back(lay, pieces, wd, chunks):
    width, depth = wd.shape
    t = tile_of(width)
    tiles = width // t
    split = split_of(tiles, chunks)
    outs = []
    for start, stop in split:
        outs += half_outs(lay, (stop - start) * t)
    scratch = [
        pltpu.VMEM((lay.rows, depth), BF16),
        pltpu.VMEM((tiles, t, depth), BF16),
        *half_scratch(lay, tiles, t),
        pltpu.SemaphoreType.DMA((tiles,)),
        pltpu.SemaphoreType.DMA((len(pieces),)),
        pltpu.SemaphoreType.DMA((tiles, lay.h)),
    ]
    body = functools.partial(back_body, lay, t, split, len(pieces))
    flops, moved = 2 * lay.rows * depth * width, 2 * depth * width
    return grouped(lay, call(body, [*pieces, wd], outs, scratch, flops, moved, direct=len(outs)))


def pull_body(lay, t, tiles, counts, *refs):
    chunks = []
    for n in counts:
        chunks.append(refs[:n])
        refs = refs[n:]
    tables, refs = refs[:4], refs[4:]
    outs = refs[: lay.cols]
    b_v, dests, acc, w_sem, in_sem = refs[lay.cols], refs[lay.cols + 1 : lay.cols + 5], *refs[-3:]
    small = start_all(load_rows(chunks, b_v, in_sem))
    loads = functools.partial(weight_copies, t, list(zip(tables, dests)), w_sem)
    each(0, tiles, lambda i: start_all(loads(i)) and None)
    acc[...] = jnp.zeros_like(acc)
    wait_all(small)
    wg_v, wu_v, s_v, a_v = dests
    shape = (lay.h, lay.q, lay.low, SUB, t)

    def one(i):
        wait_all(loads(i))
        back = b_v[:, cols_of(i, t)].astype(F32).reshape(shape)
        gp = (spread(lay, s_v[i]) * back).reshape(lay.rows, t).astype(BF16)
        up = (spread(lay, a_v[i]) * back).reshape(lay.rows, t).astype(BF16)
        acc[...] += lax.dot_general(
            wg_v[i], gp, TRANSPOSED, preferred_element_type=F32
        ) + lax.dot_general(wu_v[i], up, TRANSPOSED, preferred_element_type=F32)

    each(0, tiles, one)
    write_sum(lay, acc[...].T, outs)


def pull(lay, chunks, wg, wu, slope, act):
    depth, width = wg.shape
    t = tile_of(width)
    tiles = width // t
    pieces = [p for c in chunks for p in c]
    scratch = [
        pltpu.VMEM((lay.rows, width), BF16),
        pltpu.VMEM((tiles, depth, t), BF16),
        pltpu.VMEM((tiles, depth, t), BF16),
        pltpu.VMEM((tiles, lay.tokens, t), F32),
        pltpu.VMEM((tiles, lay.tokens, t), F32),
        pltpu.VMEM((depth, lay.rows), F32),
        pltpu.SemaphoreType.DMA((tiles, 4)),
        pltpu.SemaphoreType.DMA((len(pieces),)),
    ]
    body = functools.partial(pull_body, lay, t, tiles, [len(c) for c in chunks])
    flops, moved = 4 * lay.rows * depth * width, 4 * depth * width
    ins = [*pieces, wg, wu, slope, act]
    return call(body, ins, sum_outs(lay, depth), scratch, flops, moved)


def scatter_rows(lay, keep, sends):
    total = keep
    for k, s in enumerate(sends, 1):
        total = total + swap(s, "row", k).astype(F32)
    b = lay.block
    parts = [total[:b]]
    for k in range(1, lay.q):
        parts.append(swap(total[k * b : (k + 1) * b].astype(BF16), "row", k * lay.h).astype(F32))
    return sum(parts[1:], parts[0])


def gather_rows(lay, own):
    near = [own]
    for k in range(1, lay.q):
        near.append(swap(own, "row", k * lay.h))
    far = jnp.concatenate(near[1:], axis=0)
    for k in range(1, lay.h):
        for p in (own, far):
            near.append(swap(p, "row", k))
    return near


def scatter_cols(keep, sends):
    total = keep
    for k, s in enumerate(sends, 1):
        total = total + swap(s, "col", k).astype(F32)
    return total


def gather_cols(lay, own):
    return [own] + [swap(own, "col", k) for k in range(1, lay.cols)]


def scatter_tokens(lay, both, h):
    part = both.shape[1] // lay.h
    columns = lambda k: lax.dynamic_slice_in_dim(both, (h ^ k) * part, part, axis=1)
    total = columns(0)
    for k in range(1, lay.h):
        total = total + swap(columns(k), "row", k)
    b = 2 * SUB
    out = total[:b]
    for k in range(1, lay.q):
        out = out + swap(total[k * b : (k + 1) * b], "row", k * lay.h)
    return out


def join_columns(lay, mine, h):
    part = mine.shape[1]
    full = jnp.zeros((mine.shape[0], part * lay.h), mine.dtype)
    for k in range(lay.h):
        piece = mine if k == 0 else swap(mine, "row", k)
        full = lax.dynamic_update_slice_in_dim(full, piece, (h ^ k) * part, axis=1)
    return full


def gates_of(joined):
    both = joined.reshape(-1, 2, SUB, joined.shape[1])
    rows = both.shape[0] * SUB
    gate, up = both[:, 0].reshape(rows, -1), both[:, 1].reshape(rows, -1)
    sigmoid_gate = 1.0 / (1.0 + jnp.exp(-gate))
    act = gate * sigmoid_gate
    return sigmoid_gate * (1.0 + gate * (1.0 - sigmoid_gate)) * up, act


def local(tokens, gain, gate_weight, up_weight, down_weight, probes):
    probe_count, token_count, depth = probes.shape
    lay = Layout(probe_count, token_count, lax.axis_size("row"), lax.axis_size("col"))
    r, c = lax.axis_index("row"), lax.axis_index("col")
    h, q = r % lay.h, r // lay.h
    blocks = probe_count * lay.q
    flip = (h * (lay.q * lay.low)) ^ (q * lay.low) ^ (c * (blocks // lay.cols))
    order = jnp.arange(blocks, dtype=jnp.int32) ^ flip
    token_order = jnp.arange(lay.q, dtype=jnp.int32) ^ ((flip // lay.low) % lay.q)
    five = (lay.h, lay.low, lay.q, SUB, depth)
    gain_row = gain[None, :]

    scaled = (tokens.astype(F32) * gain_row).astype(BF16)
    scaled = scaled.reshape(lay.q, SUB, depth)[token_order].reshape(token_count, depth)
    natural = probes.reshape(five).transpose(0, 2, 1, 3, 4).reshape(blocks, SUB, depth)
    pushed = (natural[order].reshape(lay.rows, depth) * gain_row).astype(BF16)
    tok, parts = first(lay, scaled, pushed, gate_weight, up_weight, CHUNKS)
    own = scatter_tokens(lay, tok, h)
    own_slope, own_act = gates_of(join_columns(lay, own, h))
    own_slope = jnp.tile(own_slope, (lay.low, 1))
    own_act = jnp.tile(own_act, (lay.low, 1))
    levels = None
    entries = token_count * depth * lay.ranks
    for sweep in range(ITERS):
        chunks = []
        if sweep:
            parts = push(lay, pushed, gate_weight, up_weight, slope, act, levels, CHUNKS)
        at = 0
        for k, (keep, *sends) in enumerate(parts):
            if sweep == 0:
                total = scatter_rows(lay.doubled(), keep, sends)
                here = slice(at, at + total.shape[1])
                at += total.shape[1]
                total = (
                    own_slope[:, here] * total[: lay.block]
                    + own_act[:, here] * total[lay.block :]
                ).astype(BF16)
            else:
                total = scatter_rows(lay, keep, sends)
                if k == 0:
                    scale = lax.rsqrt(total[:, -128:-127] / entries + EPSILON)
                    total = total[:, :-128]
                total = (total * scale).astype(BF16)
                if k == 0:
                    total, scale = lax.optimization_barrier((total, scale))
            chunks.append(gather_rows(lay, total))
        res = down(lay, chunks, down_weight)
        tangent = scatter_cols(res[0], res[1:]).astype(BF16)
        if sweep == 0:
            tangent, own = lax.optimization_barrier((tangent, own))
            mine = [own] + [swap(own, "row", k * lay.h) for k in range(1, lay.q)]
            slope, act = gates_of(join_columns(lay, jnp.concatenate(mine, axis=0), h))
        tangents = gather_cols(lay, tangent)
        chunks = []
        parts = pull_back(lay, tangents, down_weight, CHUNKS)
        for keep, *sends in parts:
            total = scatter_rows(lay, keep, sends)
            total = total.astype(BF16)
            chunks.append(gather_rows(lay, total))
        res = pull(lay, chunks, gate_weight, up_weight, slope, act)
        pulled = scatter_cols(res[0], res[1:])
        final = sweep == ITERS - 1
        if final:
            grown = stack_rows(gather_cols(lay, pulled.astype(BF16))).astype(F32) * gain_row
        else:
            pushed = stack_rows(gather_cols(lay, (pulled * gain_row * gain_row).astype(BF16)))
            grown = pushed.astype(F32) / gain_row
        squares = jnp.sum(
            (grown * grown).reshape(lay.h, lay.q, lay.low, SUB, depth), axis=(1, 3, 4)
        )
        if final:
            outer = (flip // (lay.q * lay.low)) % lay.h
            inner = flip % lay.low
            far = (jnp.arange(lay.h) ^ outer)[:, None]
            near = (jnp.arange(lay.low) ^ inner)[None, :]
            level = squares[far, near].reshape(-1)
            mask = 1
            while mask < lay.ranks:
                level = level + swap(level, "row", mask)
                mask *= 2
            level = level / entries
            basis = grown.reshape(blocks, SUB, depth)[order]
            basis = basis.reshape(lay.h, lay.q, lay.low, SUB, depth).transpose(0, 2, 1, 3, 4)
            basis = basis.reshape(probe_count, token_count, depth)
            return basis * lax.rsqrt(level + EPSILON)[:, None, None], jnp.sqrt(level)
        levels = jnp.broadcast_to(
            squares[:, None, :, None, None], (lay.h, lay.q, lay.low, SUB, 128)
        ).reshape(lay.rows, 128)


def solution(mesh):
    placed = (
        P(None, "row"),
        P("row"),
        P("row", "col"),
        P("row", "col"),
        P("col", "row"),
        P(None, None, "row"),
    )
    return jax.shard_map(
        local, mesh=mesh, in_specs=placed, out_specs=(P(None, None, "row"), P()), check_vma=False
    )
```
